32 devices in a mesh: samp: 8 (over y, x, core), par: 4 (over z).
Axes of the slice: x: 2, y: 2, z: 4, core: 2. Of those that a mesh axis runs over, the one named last changes fastest.
Arguments:
- log_derivs: bfloat16 [512, 262144], P('samp', 'par')
- energies: float32 [512, 8], P('samp'), may hold values from -6 to 6
- nys_rows: int32 [8, 8], P('samp'), may hold values from 0 to 63, as said below
Outputs:
- update: float32 [262144, 8], P('par')
- solution: float32 [512, 8], P('samp')
The draws below stay inside these ranges and needn't reach their ends.
Inputs may be any that keep to these rules, and one draw needn't show every extreme that they name: `nys_rows`: each row holds 8 different local sample numbers of that group.
All inputs are finite; a program needn't handle non-finite values.
Results may differ from the reference program's by a relative error of at most 0.014.
Values may be sent and summed in bfloat16 or wider, within the bound.
A program may use at most 128 MiB of HBM per device.

```python
import math
import jax
import jax.numpy as jnp
from jax import lax

SAMP_DEV = 64
PAR_DEV = 65536
NV = 8
RANK_DEV = 8
ITERS = 2
GROUPS = 8
NS = 512
NP = 262144
RANK = 64
N_PAR = 4


def draw_log_derivs(key, part):
    subkeys = jax.random.split(jax.random.fold_in(key, 11), 6)
    row_scale = jnp.exp(jax.random.uniform(subkeys[0], (NS, 1), jnp.float32, 0.0, math.log(10.0)))
    col_scale = jnp.exp(jax.random.uniform(subkeys[1], (1, NP), jnp.float32, math.log(0.5), math.log(2.0)))
    offset = 2.0 * jax.random.normal(subkeys[2], (1, NP), jnp.float32)
    latent_count = max(NS // 8, 8)
    latent = jax.random.normal(subkeys[4], (NS, latent_count), jnp.float32)
    loading = jax.random.normal(subkeys[5], (latent_count, NP), jnp.float32) * (0.5 / math.sqrt(latent_count))
    shared = jnp.dot(latent, loading)
    fluctuation = jax.random.normal(subkeys[3], (NS, NP), jnp.float32)
    return (offset + row_scale * (col_scale * fluctuation + shared)).astype(jnp.bfloat16)


def draw_nys_rows(key, part):
    subkeys = jax.random.split(jax.random.fold_in(key, 7), GROUPS)

    def pick_rows(subkey):
        return jax.random.permutation(subkey, SAMP_DEV)[:RANK_DEV]
    return jax.vmap(pick_rows)(subkeys).astype(jnp.int32)


def block_levels(own_key, extent, cuts, low, top_value):
    factor_of, own = 1.0, jax.random.fold_in(own_key, 6)
    for position, shards_of in cuts:
        heights = jnp.exp(jax.random.uniform(jax.random.fold_in(own, position), (shards_of,), jnp.float32, low / len(cuts), top_value / len(cuts)))
        factor_of = factor_of * jnp.repeat(heights, extent[position] // shards_of).reshape([-1 if axis == position else 1 for axis in range(len(extent))])
    return factor_of


def scatter_about(stream_key, extent, spread, bound, cuts=(), kind=jnp.bfloat16):
    gain = block_levels(stream_key, extent, cuts, -0.22, 0.18) if cuts else 1.0
    drawn = jax.random.normal(stream_key, extent, jnp.float32) * spread * gain
    return jnp.minimum(jnp.maximum(drawn, -bound), bound).astype(kind)


def setup_inputs(seed: int = 0) -> dict:
    splits = jax.random.split(jax.random.key(seed), 4)
    log_derivs = draw_log_derivs(jax.random.fold_in(splits[3], 71), 0)
    energies = scatter_about(splits[1], (NS, NV), 1.0, 6.0, ((0, 8),), jnp.float32)
    nys_rows = draw_nys_rows(jax.random.fold_in(splits[3], 71), 0)
    return {"log_derivs": log_derivs, "energies": energies, "nys_rows": nys_rows}


damping = 0.5

def centered_block(log_derivs, index):
    block = lax.dynamic_slice_in_dim(log_derivs, (index * PAR_DEV).astype(jnp.int32), PAR_DEV, 1).astype(jnp.float32)
    column_mean = lax.optimization_barrier(jnp.sum(block, axis=0)) / NS
    return ((block - column_mean) * (1.0 / math.sqrt(NP))).astype(jnp.bfloat16)

def factor_solve(factor, right):
    middle = lax.linalg.triangular_solve(factor, right, left_side=True, lower=True)
    return lax.linalg.triangular_solve(factor, middle, left_side=True, lower=True, transpose_a=True)

def small_solve(matrix, right):
    return factor_solve(jnp.linalg.cholesky(matrix), right)

def hdot(left, right):
    return jnp.dot(left, right, precision=lax.Precision.HIGHEST)

def reference(log_derivs, energies, nys_rows):
    selected = (jnp.arange(GROUPS, dtype=jnp.int32)[:, None] * SAMP_DEV + nys_rows).reshape(-1).astype(jnp.int32)
    indices = jnp.arange(N_PAR, dtype=jnp.int32)

    def add_sketch(total, index):
        block = centered_block(log_derivs, index)
        chosen = jnp.take(block, selected, axis=0)
        return (total + jnp.dot(block.astype(jnp.float32), chosen.T.astype(jnp.float32), preferred_element_type=jnp.float32), None)
    sketch, unused = lax.scan(add_sketch, jnp.zeros((NS, RANK), jnp.float32), indices)
    core_block = jnp.take(sketch, selected, axis=0)
    inner_matrix = damping * core_block + hdot(sketch.T, sketch)
    factor = jnp.linalg.cholesky(inner_matrix)

    def precondition(residual):
        coeffs = factor_solve(factor, hdot(sketch.T, residual))
        result = (residual - hdot(sketch, coeffs)) / damping
        return (result, hdot(result.T, residual))

    def apply_kernel(direction):
        rounded = direction.astype(jnp.bfloat16)

        def add_image(total, index):
            block = centered_block(log_derivs, index)
            projected = jnp.dot(block.T.astype(jnp.float32), rounded.astype(jnp.float32), preferred_element_type=jnp.float32)
            return (total + hdot(block.astype(jnp.float32), projected), None)
        images, unused_two = lax.scan(add_image, jnp.zeros((NS, NV), jnp.float32), indices)
        return images + damping * direction
    solution = jnp.zeros((NS, NV), jnp.float32)
    residual = energies
    precond_res, inner_prev = precondition(residual)
    direction = precond_res
    for iteration in range(ITERS):
        image_k = apply_kernel(direction)
        curvature = hdot(direction.T, image_k)
        alpha_k = small_solve(curvature, inner_prev)
        solution = solution + hdot(direction, alpha_k)
        if iteration + 1 < ITERS:
            residual = residual - hdot(image_k, alpha_k)
            precond_res, inner_next = precondition(residual)
            beta_k = small_solve(inner_prev, inner_next)
            direction = precond_res + hdot(direction, beta_k)
            inner_prev = inner_next
    rounded_sol = solution.astype(jnp.bfloat16)

    def update_block(index):
        block = centered_block(log_derivs, index)
        return jnp.dot(block.T.astype(jnp.float32), rounded_sol.astype(jnp.float32), preferred_element_type=jnp.float32)
    update = lax.map(update_block, indices).reshape(NP, NV)
    return (update, solution)
```

```python
import functools
import math

import jax
import jax.numpy as jnp
from jax import lax
from jax.experimental import pallas as pl
from jax.experimental.pallas import tpu as pltpu
from jax.sharding import PartitionSpec as P

ITERS = 2


damping = 0.5

MESH = pl.DeviceIdType.MESH


def factor_solve(factor, right):
    middle = lax.linalg.triangular_solve(factor, right, left_side=True, lower=True)
    return lax.linalg.triangular_solve(factor, middle, left_side=True, lower=True, transpose_a=True)


def small_solve(matrix, right):
    return factor_solve(jnp.linalg.cholesky(matrix), right)


def hdot(left, right):
    return jnp.dot(left, right, precision=lax.Precision.HIGHEST)


def greet(peers):
    barrier = pltpu.get_barrier_semaphore()
    for peer in peers:
        pl.semaphore_signal(barrier, inc=1, device_id=peer, device_id_type=MESH)
    pl.semaphore_wait(barrier, len(peers))


def remote(src, dst, send, recv, peer):
    return pltpu.make_async_remote_copy(
        src_ref=src, dst_ref=dst, send_sem=send, recv_sem=recv, device_id=peer, device_id_type=MESH
    )


def gather_kernel(n, total_rows, sums_ref, aux_ref, chosen_ref, mean_ref, aux_out, rows_out,
                  land, own, s1, r1, s2, r2, s3, r3, s4, r4, s5, r5, local):
    me, col = lax.axis_index("samp"), lax.axis_index("par")
    at = [lax.rem(me + k, n) for k in range(n)]
    back = [lax.rem(me + n - k, n) for k in range(n)]
    peer = [(at[k], col) for k in range(n)]
    pair = jnp.bitwise_xor(me, 1)
    greet(peer[1:])
    scatter = [remote(sums_ref.at[at[k]], land.at[k], s1.at[k], r1.at[k], peer[k]) for k in range(1, n)]
    for copy in scatter:
        copy.start()
    auxes = [remote(aux_ref, aux_out.at[me], s2.at[k], r2.at[k], peer[k]) for k in range(1, n)]
    for copy in auxes:
        copy.start()
    mine = pltpu.make_async_copy(aux_ref, aux_out.at[me], local.at[0])
    mine.start()
    keep = pltpu.make_async_copy(chosen_ref, rows_out.at[me], local.at[1])
    keep.start()
    total = sums_ref[me]
    for k in range(1, n):
        scatter[k - 1].wait_recv()
        total = total + land[k]
    own[...] = total / total_rows
    mean_ref[me] = own[...]
    spread = [remote(own, mean_ref.at[me], s3.at[k], r3.at[k], peer[k]) for k in range(1, n)]
    for copy in spread:
        copy.start()
    far = [remote(chosen_ref, rows_out.at[me], s4.at[k], r4.at[k], peer[k]) for k in range(2, n, 2)]
    for copy in far:
        copy.start()
    over = [remote(chosen_ref, rows_out.at[me], s5.at[0], r5.at[0], (pair, col))]
    over[0].start()
    for i, k in enumerate(range(2, n, 2)):
        remote(
            chosen_ref, rows_out.at[back[k]], s4.at[k], r4.at[k], peer[k]).wait_recv()
        step = remote(rows_out.at[back[k]], rows_out.at[back[k]], s5.at[k], r5.at[k], (pair, col))
        step.start()
        over.append(step)
    for i, k in enumerate(range(0, n, 2)):
        source = lax.rem(pair + n - k, n)
        remote(chosen_ref, rows_out.at[source], s5.at[k], r5.at[k], (pair, col)).wait_recv()
    for k in range(1, n):
        remote(aux_ref, aux_out.at[back[k]], s2.at[k], r2.at[k], peer[k]).wait_recv()
        remote(own, mean_ref.at[back[k]], s3.at[k], r3.at[k], peer[k]).wait_recv()
    for copy in scatter + auxes + spread + far + over:
        copy.wait_send()
    mine.wait()
    keep.wait()


def gather_rows(sums, aux, chosen, n, total_rows, ident):
    dma = lambda: pltpu.SemaphoreType.DMA((n,))
    vmem = pl.BlockSpec(memory_space=pltpu.VMEM)
    slab = sums.shape[-1]
    return pl.pallas_call(
        functools.partial(gather_kernel, n, total_rows),
        out_shape=(
            jax.ShapeDtypeStruct(sums.shape, jnp.float32),
            jax.ShapeDtypeStruct((n,) + aux.shape, jnp.float32),
            jax.ShapeDtypeStruct((n,) + chosen.shape, chosen.dtype),
        ),
        in_specs=[vmem, vmem, vmem],
        out_specs=(vmem, vmem, vmem),
        scratch_shapes=[
            pltpu.VMEM(sums.shape, jnp.float32),
            pltpu.VMEM((1, slab), jnp.float32),
        ] + [dma() for _ in range(10)] + [pltpu.SemaphoreType.DMA((2,))],
        compiler_params=pltpu.CompilerParams(
            collective_id=ident, has_side_effects=True, vmem_limit_bytes=48 * 2**20
        ),
    )(sums, aux, chosen)


def spread_kernel(n, p, part_ref, out_ref, land, own, s1, r1, s2, r2):
    me, col = lax.axis_index("samp"), lax.axis_index("par")
    flat, size = me * p + col, n * p
    barrier = pltpu.get_barrier_semaphore()

    def place(k):
        there = lax.rem(flat + k, size)
        return (there // p, lax.rem(there, p))

    @pl.loop(1, size)
    def _(k):
        pl.semaphore_signal(barrier, inc=1, device_id=place(k), device_id_type=MESH)

    pl.semaphore_wait(barrier, size - 1)
    sums = []
    for k in range(1, p):
        there = lax.rem(col + k, p)
        sums.append(remote(part_ref.at[there], land.at[k], s1.at[k], r1.at[k], (me, there)))
        sums[-1].start()
    total = part_ref[col]
    for k in range(1, p):
        sums[k - 1].wait_recv()
        total = total + land[k]
    own[...] = total
    out_ref[flat] = total

    def hop(k, slot):
        return remote(own, out_ref.at[slot], s2.at[k], r2.at[k], place(k))

    @pl.loop(1, size)
    def _(k):
        hop(k, flat).start()

    @pl.loop(1, size)
    def _(k):
        hop(k, lax.rem(flat + size - k, size)).wait_recv()

    @pl.loop(1, size)
    def _(k):
        hop(k, flat).wait_send()

    for copy in sums:
        copy.wait_send()


def sum_and_spread(part, n, p, ident):
    rows, width = part.shape
    cut = part.reshape(p, rows // p, width)
    vmem = pl.BlockSpec(memory_space=pltpu.VMEM)
    out = pl.pallas_call(
        functools.partial(spread_kernel, n, p),
        out_shape=jax.ShapeDtypeStruct((n * p, rows // p, width), jnp.float32),
        in_specs=[vmem],
        out_specs=vmem,
        scratch_shapes=[
            pltpu.VMEM(cut.shape, jnp.float32),
            pltpu.VMEM(cut.shape[1:], jnp.float32),
            pltpu.SemaphoreType.DMA((p,)),
            pltpu.SemaphoreType.DMA((p,)),
            pltpu.SemaphoreType.DMA((n * p,)),
            pltpu.SemaphoreType.DMA((n * p,)),
        ],
        compiler_params=pltpu.CompilerParams(collective_id=ident, has_side_effects=True),
    )(cut)
    return out.reshape(n * rows, width)


def reduce_kernel(n, part_ref, out_ref, land, s1, r1, s2, r2):
    me, col = lax.axis_index("samp"), lax.axis_index("par")
    slab = land.shape[-1]
    at = [lax.rem(me + k, n) for k in range(n)]
    back = [lax.rem(me + n - k, n) for k in range(n)]
    peer = [(at[k], col) for k in range(n)]
    cols = lambda j: pl.ds(pl.multiple_of(j * slab, slab), slab)
    greet(peer[1:])
    scatter = [
        remote(part_ref.at[:, cols(at[k])], land.at[k], s1.at[k], r1.at[k], peer[k]) for k in range(1, n)
    ]
    for copy in scatter:
        copy.start()
    total = part_ref[:, cols(me)].astype(jnp.float32)
    for k in range(1, n):
        scatter[k - 1].wait_recv()
        total = total + land[k].astype(jnp.float32)
    out_ref[:, cols(me)] = total.astype(out_ref.dtype)
    spread = [
        remote(out_ref.at[:, cols(me)], out_ref.at[:, cols(me)], s2.at[k], r2.at[k], peer[k])
        for k in range(1, n)
    ]
    for copy in spread:
        copy.start()
    for k in range(1, n):
        remote(out_ref.at[:, cols(me)], out_ref.at[:, cols(back[k])], s2.at[k], r2.at[k], peer[k]).wait_recv()
    for copy in scatter + spread:
        copy.wait_send()


def reduce_all(part, n, ident):
    count, width = part.shape
    vmem = pl.BlockSpec(memory_space=pltpu.VMEM)
    return pl.pallas_call(
        functools.partial(reduce_kernel, n),
        out_shape=jax.ShapeDtypeStruct(part.shape, part.dtype),
        in_specs=[vmem],
        out_specs=vmem,
        scratch_shapes=[pltpu.VMEM((n, count, width // n), part.dtype)]
        + [pltpu.SemaphoreType.DMA((n,)) for _ in range(4)],
        compiler_params=pltpu.CompilerParams(collective_id=ident, has_side_effects=True),
    )(part)


def tiny_kernel(p, part_ref, out_ref, land, s1, r1):
    me, col = lax.axis_index("samp"), lax.axis_index("par")
    at = [lax.rem(col + k, p) for k in range(p)]
    back = [lax.rem(col + p - k, p) for k in range(p)]
    greet([(me, at[k]) for k in range(1, p)])
    copies = [remote(part_ref, land.at[col], s1.at[k], r1.at[k], (me, at[k])) for k in range(1, p)]
    for copy in copies:
        copy.start()
    land[col] = part_ref[...]
    for k in range(1, p):
        remote(part_ref, land.at[back[k]], s1.at[k], r1.at[k], (me, at[k])).wait_recv()
    for copy in copies:
        copy.wait_send()
    total = land[0]
    for j in range(1, p):
        total = total + land[j]
    out_ref[...] = total


def tiny_sum(part, p, ident):
    vmem = pl.BlockSpec(memory_space=pltpu.VMEM)
    return pl.pallas_call(
        functools.partial(tiny_kernel, p),
        out_shape=jax.ShapeDtypeStruct(part.shape, part.dtype),
        in_specs=[vmem],
        out_specs=vmem,
        scratch_shapes=[pltpu.VMEM((p,) + part.shape, part.dtype)]
        + [pltpu.SemaphoreType.DMA((p,)) for _ in range(2)],
        compiler_params=pltpu.CompilerParams(collective_id=ident, has_side_effects=True),
    )(part)


def body(log_derivs, energies, nys_rows):
    rows, width = log_derivs.shape
    n, p = lax.axis_size("samp"), lax.axis_size("par")
    count, rank = energies.shape[1], nys_rows.shape[1]
    scale = 1.0 / math.sqrt(width * p)
    picks = (nys_rows.reshape(rank, 1) == lax.broadcasted_iota(jnp.int32, (rank, rows), 1)).astype(jnp.bfloat16)
    probe = jnp.concatenate([picks, jnp.ones((8, rows), jnp.bfloat16)], axis=0)
    taken = jnp.dot(probe, log_derivs, preferred_element_type=jnp.float32)
    chosen = taken[:rank].astype(jnp.bfloat16)
    sums = taken[rank].reshape(n, 1, width // n)
    aux = jnp.concatenate([energies, picks.astype(jnp.float32).T], axis=1)
    mean, aux_all, chosen_all = gather_rows(sums, aux, chosen, n, n * rows, 0)
    mean = mean.reshape(1, width)
    centered = ((log_derivs.astype(jnp.float32) - mean) * scale).astype(jnp.bfloat16)
    chosen_all = chosen_all.reshape(n * rank, width)
    chosen_all = ((chosen_all.astype(jnp.float32) - mean) * scale).astype(jnp.bfloat16)
    sketch_part = jnp.einsum("rc,kc->rk", centered, chosen_all, preferred_element_type=jnp.float32)
    sketch = sum_and_spread(sketch_part, n, p, 1)
    all_energies = aux_all[:, :, :count].reshape(n * rows, count)
    core_block = jnp.einsum(
        "grj,grk->gjk", aux_all[:, :, count:], sketch.reshape(n, rows, n * rank), precision=lax.Precision.HIGHEST
    ).reshape(n * rank, n * rank)
    factor = jnp.linalg.cholesky(damping * core_block + hdot(sketch.T, sketch))

    def precondition(residual):
        coeffs = factor_solve(factor, hdot(sketch.T, residual))
        result = (residual - hdot(sketch, coeffs)) / damping
        return (result, hdot(result.T, residual))

    start = lax.axis_index("samp") * rows
    solution = jnp.zeros(all_energies.shape, jnp.float32)
    update = 0.0
    residual = all_energies
    precond_res, inner_prev = precondition(residual)
    direction = precond_res
    for iteration in range(ITERS):
        rounded = lax.dynamic_slice_in_dim(direction, start, rows, 0).astype(jnp.bfloat16)
        part = jnp.einsum("rv,rc->vc", rounded, centered, preferred_element_type=jnp.float32)
        projected = reduce_all(part.astype(jnp.bfloat16), n, 2 + 2 * iteration)
        if iteration + 1 < ITERS:
            image_part = jnp.einsum("rc,vc->rv", centered, projected, preferred_element_type=jnp.float32)
            image_k = sum_and_spread(image_part, n, p, 3 + 2 * iteration) + damping * direction
            curvature = hdot(direction.T, image_k)
        else:
            square = jnp.einsum("uc,vc->uv", projected, projected, preferred_element_type=jnp.float32)
            curvature = tiny_sum(square, p, 3 + 2 * iteration) + damping * hdot(direction.T, direction)
        alpha_k = small_solve(curvature, inner_prev)
        solution = solution + hdot(direction, alpha_k)
        update = update + hdot(alpha_k.T, projected.astype(jnp.float32))
        if iteration + 1 < ITERS:
            residual = residual - hdot(image_k, alpha_k)
            precond_res, inner_next = precondition(residual)
            beta_k = small_solve(inner_prev, inner_next)
            direction = precond_res + hdot(direction, beta_k)
            inner_prev = inner_next
    return (update.T, lax.dynamic_slice_in_dim(solution, start, rows, 0))


def solution(mesh):
    return jax.shard_map(
        body,
        mesh=mesh,
        in_specs=(P("samp", "par"), P("samp", None), P("samp", None)),
        out_specs=(P("par", None), P("samp", None)),
        check_vma=False,
    )
```

```python
import functools
import math

import jax
import jax.numpy as jnp
from jax import lax
from jax.experimental import pallas as pl
from jax.experimental.pallas import tpu as pltpu
from jax.sharding import PartitionSpec as P

ITERS = 2


damping = 0.5

MESH = pl.DeviceIdType.MESH


def factor_solve(factor, right):
    middle = lax.linalg.triangular_solve(factor, right, left_side=True, lower=True)
    return lax.linalg.triangular_solve(factor, middle, left_side=True, lower=True, transpose_a=True)


def eliminate_kernel(matrix_ref, right_ref, out_ref):
    left, right = matrix_ref[...], right_ref[...]
    row = lax.broadcasted_iota(jnp.int32, left.shape, 0)
    for i in range(left.shape[0]):
        column = left[:, i:i + 1]
        pivot = left[i:i + 1, i:i + 1]
        left_row = left[i:i + 1, :] / pivot
        right_row = right[i:i + 1, :] / pivot
        left = jnp.where(row == i, left_row, left - column * left_row)
        right = jnp.where(row == i, right_row, right - column * right_row)
    out_ref[...] = right


def small_solve(matrix, right):
    matrix = 0.5 * (matrix + matrix.T)
    return pl.pallas_call(
        eliminate_kernel, out_shape=jax.ShapeDtypeStruct(right.shape, right.dtype)
    )(matrix, right)


def hdot(left, right):
    return jnp.dot(left, right, precision=lax.Precision.HIGHEST)


def greet(peers):
    barrier = pltpu.get_barrier_semaphore()
    for peer in peers:
        pl.semaphore_signal(barrier, inc=1, device_id=peer, device_id_type=MESH)
    pl.semaphore_wait(barrier, len(peers))


def remote(src, dst, send, recv, peer):
    return pltpu.make_async_remote_copy(
        src_ref=src, dst_ref=dst, send_sem=send, recv_sem=recv, device_id=peer, device_id_type=MESH
    )


def gather_kernel(n, total_rows, scale, sums_ref, aux_ref, chosen_ref, full_ref, mean_ref, aux_out, rows_out, centered_ref,
                  land, own, full, s1, r1, s2, r2, s3, r3, s4, r4, s5, r5, s6, r6, local):
    me, col = lax.axis_index("samp"), lax.axis_index("par")
    at = [lax.rem(me + k, n) for k in range(n)]
    back = [lax.rem(me + n - k, n) for k in range(n)]
    peer = [(at[k], col) for k in range(n)]
    pair = (jnp.bitwise_xor(me, 1), col)
    width = chosen_ref.shape[1]
    half = width // 2
    part = [pl.ds(0, half), pl.ds(half, half)]
    load = pltpu.make_async_copy(full_ref, full, local.at[2])
    load.start()
    greet(peer[1:])
    scatter = [remote(sums_ref.at[at[k]], land.at[k], s1.at[k], r1.at[k], peer[k]) for k in range(1, n)]
    for copy in scatter:
        copy.start()
    sent = list(scatter)
    quad = n == 8
    beside = [jnp.bitwise_xor(me, 2), jnp.bitwise_xor(me, 4)]
    if quad:
        first = [
            remote(chosen_ref.at[:, part[d]], rows_out.at[me, :, part[d]], s4.at[d], r4.at[d], (beside[d], col))
            for d in range(2)
        ]
        for copy in first:
            copy.start()
        sent += first
    auxes = [remote(aux_ref, aux_out.at[me], s2.at[k], r2.at[k], peer[k]) for k in range(1, n)]
    mine = pltpu.make_async_copy(aux_ref, aux_out.at[me], local.at[0])
    mine.start()
    keep = pltpu.make_async_copy(chosen_ref, rows_out.at[me], local.at[1])
    keep.start()
    total = sums_ref[me]
    for k in range(1, n):
        scatter[k - 1].wait_recv()
        total = total + land[k]
    own[...] = total / total_rows
    mean_ref[me] = own[...]
    spread = [remote(own, mean_ref.at[me], s3.at[k], r3.at[k], peer[k]) for k in range(1, n)]
    for copy in spread + auxes:
        copy.start()
    sent += spread + auxes
    over = [remote(chosen_ref, rows_out.at[me], s5.at[0], r5.at[0], pair)]
    over[0].start()
    if quad:
        second = [
            remote(chosen_ref.at[:, part[1 - d]], rows_out.at[me, :, part[1 - d]], s4.at[2 + d], r4.at[2 + d],
                   (beside[d], col))
            for d in range(2)
        ]
        for copy in second:
            copy.start()
        sent += second
        for d in range(2):
            view = rows_out.at[beside[d], :, part[d]]
            remote(view, view, s4.at[d], r4.at[d], pair).wait_recv()
            step = remote(view, view, s4.at[4 + d], r4.at[4 + d], (beside[1 - d], col))
            step.start()
            sent.append(step)
    else:
        far = [remote(chosen_ref, rows_out.at[me], s4.at[k], r4.at[k], peer[k]) for k in range(2, n, 2)]
        for copy in far:
            copy.start()
        sent += far
    for k in range(1, n):
        remote(own, mean_ref.at[back[k]], s3.at[k], r3.at[k], peer[k]).wait_recv()
    load.wait()
    slab = width // n
    tile = math.gcd(slab, 1024)

    @pl.loop(0, n)
    def _(j):
        @pl.loop(0, slab // tile)
        def _(t):
            inner = pl.multiple_of(t * tile, tile)
            cols = pl.ds(pl.multiple_of(j * slab + inner, tile), tile)
            mean = mean_ref[j, :, pl.ds(inner, tile)]
            centered_ref[:, cols] = ((full[:, cols].astype(jnp.float32) - mean) * scale).astype(jnp.bfloat16)

    if quad:
        for d in range(2):
            view = rows_out.at[beside[d], :, part[1 - d]]
            remote(view, view, s4.at[2 + d], r4.at[2 + d], pair).wait_recv()
            block = rows_out.at[beside[d]]
            step = remote(block, block, s5.at[1 + d], r5.at[1 + d], pair)
            step.start()
            over.append(step)
        cross = jnp.bitwise_xor(me, 6)
        for d in range(2):
            view = rows_out.at[cross, :, part[d]]
            remote(view, view, s4.at[4 + d], r4.at[4 + d], pair).wait_recv()
            step = remote(view, view, s5.at[3 + d], r5.at[3 + d], pair)
            step.start()
            over.append(step)
        block = rows_out.at[jnp.bitwise_xor(me, 1)]
        remote(block, block, s5.at[0], r5.at[0], pair).wait_recv()
        for d in range(2):
            block = rows_out.at[jnp.bitwise_xor(me, 3 + 2 * d)]
            remote(block, block, s5.at[1 + d], r5.at[1 + d], pair).wait_recv()
            view = rows_out.at[jnp.bitwise_xor(me, 7), :, part[d]]
            remote(view, view, s5.at[3 + d], r5.at[3 + d], pair).wait_recv()
    else:
        for k in range(2, n, 2):
            block = rows_out.at[back[k]]
            remote(block, block, s4.at[k], r4.at[k], pair).wait_recv()
            step = remote(block, block, s5.at[k], r5.at[k], pair)
            step.start()
            over.append(step)
        for k in range(0, n, 2):
            block = rows_out.at[lax.rem(pair[0] + n - k, n)]
            remote(block, block, s5.at[k], r5.at[k], pair).wait_recv()
    for k in range(1, n):
        remote(aux_ref, aux_out.at[back[k]], s2.at[k], r2.at[k], peer[k]).wait_recv()
    for copy in sent + over:
        copy.wait_send()
    mine.wait()
    keep.wait()


def gather_rows(sums, aux, chosen, full, n, total_rows, scale, ident):
    dma = lambda: pltpu.SemaphoreType.DMA((n,))
    vmem = pl.BlockSpec(memory_space=pltpu.VMEM)
    slab = sums.shape[-1]
    return pl.pallas_call(
        functools.partial(gather_kernel, n, total_rows, scale),
        out_shape=(
            jax.ShapeDtypeStruct(sums.shape, jnp.float32),
            jax.ShapeDtypeStruct((n,) + aux.shape, jnp.float32),
            jax.ShapeDtypeStruct((n,) + chosen.shape, chosen.dtype),
            jax.ShapeDtypeStruct(full.shape, full.dtype),
        ),
        in_specs=[vmem, vmem, vmem, pl.BlockSpec(memory_space=pl.ANY)],
        out_specs=(vmem, vmem, vmem, vmem),
        scratch_shapes=[
            pltpu.VMEM(sums.shape, jnp.float32),
            pltpu.VMEM((1, slab), jnp.float32),
            pltpu.VMEM(full.shape, full.dtype),
        ] + [dma() for _ in range(12)] + [pltpu.SemaphoreType.DMA((3,))],
        compiler_params=pltpu.CompilerParams(
            collective_id=ident, has_side_effects=True, vmem_limit_bytes=60 * 2**20
        ),
    )(sums, aux, chosen, full)


def spread_kernel(n, p, part_ref, out_ref, land, own, s1, r1, s2, r2):
    me, col = lax.axis_index("samp"), lax.axis_index("par")
    beside = [lax.rem(col + k, p) for k in range(p)]
    at = [lax.rem(me + k, n) for k in range(n)]
    back = [lax.rem(me + n - k, n) for k in range(n)]
    greet([(me, beside[k]) for k in range(1, p)] + [(at[k], col) for k in range(1, n)])
    sums = [remote(part_ref, land.at[col], s1.at[k], r1.at[k], (me, beside[k])) for k in range(1, p)]
    for copy in sums:
        copy.start()
    land[col] = part_ref[...]
    for k in range(1, p):
        there = lax.rem(col + p - k, p)
        remote(part_ref, land.at[there], s1.at[k], r1.at[k], (me, beside[k])).wait_recv()
    total = land[0]
    for j in range(1, p):
        total = total + land[j]
    own[...] = total
    out_ref[me] = total
    hops = [remote(own, out_ref.at[me], s2.at[k], r2.at[k], (at[k], col)) for k in range(1, n)]
    for copy in hops:
        copy.start()
    for k in range(1, n):
        remote(own, out_ref.at[back[k]], s2.at[k], r2.at[k], (at[k], col)).wait_recv()
    for copy in sums + hops:
        copy.wait_send()


def sum_and_spread(part, n, p, ident):
    vmem = pl.BlockSpec(memory_space=pltpu.VMEM)
    return pl.pallas_call(
        functools.partial(spread_kernel, n, p),
        out_shape=jax.ShapeDtypeStruct((n,) + part.shape, jnp.float32),
        in_specs=[vmem],
        out_specs=vmem,
        scratch_shapes=[
            pltpu.VMEM((p,) + part.shape, jnp.float32),
            pltpu.VMEM(part.shape, jnp.float32),
            pltpu.SemaphoreType.DMA((p,)),
            pltpu.SemaphoreType.DMA((p,)),
            pltpu.SemaphoreType.DMA((n,)),
            pltpu.SemaphoreType.DMA((n,)),
        ],
        compiler_params=pltpu.CompilerParams(collective_id=ident, has_side_effects=True),
    )(part)


def reduce_kernel(n, part_ref, out_ref, land, both, inbox, s0, r0, s1, r1, s2, r2, s3, r3):
    me, col = lax.axis_index("samp"), lax.axis_index("par")
    outer = n // 2
    slab = part_ref.shape[1] // n
    half = slab * outer
    i, o = lax.rem(me, 2), me // 2
    pair = (jnp.bitwise_xor(me, 1), col)
    at = [lax.rem(o + k, outer) for k in range(outer)]
    back = [lax.rem(o + outer - k, outer) for k in range(outer)]
    peer = [(at[k] * 2 + i, col) for k in range(outer)]
    cols = lambda j: pl.ds(pl.multiple_of(j * slab, slab), slab)
    halves = lambda j: pl.ds(pl.multiple_of(j * half, half), half)
    greet([pair] + peer[1:])
    swap = remote(part_ref.at[:, halves(1 - i)], land, s0.at[0], r0.at[0], pair)
    swap.start()
    swap.wait_recv()
    both[...] = (part_ref[:, halves(i)].astype(jnp.float32) + land[...].astype(jnp.float32)).astype(both.dtype)
    scatter = [remote(both.at[:, cols(at[k])], inbox.at[k], s1.at[k], r1.at[k], peer[k]) for k in range(1, outer)]
    for copy in scatter:
        copy.start()
    total = part_ref[:, cols(i * outer + o)].astype(jnp.float32) + land[:, cols(o)].astype(jnp.float32)
    for k in range(1, outer):
        scatter[k - 1].wait_recv()
        total = total + inbox[k].astype(jnp.float32)
    home = cols(i * outer + o)
    out_ref[:, home] = total.astype(out_ref.dtype)
    mine = out_ref.at[:, home]
    spread = [remote(mine, mine, s2.at[k], r2.at[k], peer[k]) for k in range(1, outer)]
    spread.append(remote(mine, mine, s3.at[0], r3.at[0], pair))
    for copy in spread:
        copy.start()
    for k in range(1, outer):
        block = out_ref.at[:, cols(i * outer + back[k])]
        remote(block, block, s2.at[k], r2.at[k], pair).wait_recv()
        step = remote(block, block, s3.at[k], r3.at[k], pair)
        step.start()
        spread.append(step)
    for k in range(outer):
        block = out_ref.at[:, cols((1 - i) * outer + back[k])]
        remote(block, block, s3.at[k], r3.at[k], pair).wait_recv()
    for copy in [swap] + scatter + spread:
        copy.wait_send()


def reduce_all(part, n, ident):
    count, width = part.shape
    outer = n // 2
    vmem = pl.BlockSpec(memory_space=pltpu.VMEM)
    return pl.pallas_call(
        functools.partial(reduce_kernel, n),
        out_shape=jax.ShapeDtypeStruct(part.shape, part.dtype),
        in_specs=[vmem],
        out_specs=vmem,
        scratch_shapes=[
            pltpu.VMEM((count, width // 2), part.dtype),
            pltpu.VMEM((count, width // 2), part.dtype),
            pltpu.VMEM((outer, count, width // n), part.dtype),
        ]
        + [pltpu.SemaphoreType.DMA((outer,)) for _ in range(8)],
        compiler_params=pltpu.CompilerParams(collective_id=ident, has_side_effects=True),
    )(part)


def tiny_kernel(p, part_ref, out_ref, land, s1, r1):
    me, col = lax.axis_index("samp"), lax.axis_index("par")
    at = [lax.rem(col + k, p) for k in range(p)]
    back = [lax.rem(col + p - k, p) for k in range(p)]
    greet([(me, at[k]) for k in range(1, p)])
    copies = [remote(part_ref, land.at[col], s1.at[k], r1.at[k], (me, at[k])) for k in range(1, p)]
    for copy in copies:
        copy.start()
    land[col] = part_ref[...]
    for k in range(1, p):
        remote(part_ref, land.at[back[k]], s1.at[k], r1.at[k], (me, at[k])).wait_recv()
    for copy in copies:
        copy.wait_send()
    total = land[0]
    for j in range(1, p):
        total = total + land[j]
    out_ref[...] = total


def tiny_sum(part, p, ident):
    vmem = pl.BlockSpec(memory_space=pltpu.VMEM)
    return pl.pallas_call(
        functools.partial(tiny_kernel, p),
        out_shape=jax.ShapeDtypeStruct(part.shape, part.dtype),
        in_specs=[vmem],
        out_specs=vmem,
        scratch_shapes=[pltpu.VMEM((p,) + part.shape, part.dtype)]
        + [pltpu.SemaphoreType.DMA((p,)) for _ in range(2)],
        compiler_params=pltpu.CompilerParams(collective_id=ident, has_side_effects=True),
    )(part)


def body(log_derivs, energies, nys_rows):
    rows, width = log_derivs.shape
    n, p = lax.axis_size("samp"), lax.axis_size("par")
    count, rank = energies.shape[1], nys_rows.shape[1]
    scale = 1.0 / math.sqrt(width * p)
    picks = (nys_rows.reshape(rank, 1) == lax.broadcasted_iota(jnp.int32, (rank, rows), 1)).astype(jnp.bfloat16)
    probe = jnp.concatenate([picks, jnp.ones((8, rows), jnp.bfloat16)], axis=0)
    taken = jnp.dot(probe, log_derivs, preferred_element_type=jnp.float32)
    chosen = taken[:rank].astype(jnp.bfloat16)
    sums = taken[rank].reshape(n, 1, width // n)
    aux = jnp.concatenate([energies, picks.astype(jnp.float32).T], axis=1)
    mean, aux_all, chosen_all, centered = gather_rows(sums, aux, chosen, log_derivs, n, n * rows, scale, 0)
    mean = mean.reshape(1, width)
    chosen_all = chosen_all.reshape(n * rank, width)
    chosen_all = ((chosen_all.astype(jnp.float32) - mean) * scale).astype(jnp.bfloat16)
    sketch_part = jnp.einsum("rc,kc->rk", centered, chosen_all, preferred_element_type=jnp.float32)
    sketch = sum_and_spread(sketch_part, n, p, 1).reshape(n * rows, n * rank)
    all_energies = aux_all[:, :, :count].reshape(n * rows, count)
    core_block = jnp.einsum(
        "grj,grk->gjk", aux_all[:, :, count:], sketch.reshape(n, rows, n * rank), precision=lax.Precision.HIGHEST
    ).reshape(n * rank, n * rank)
    factor = jnp.linalg.cholesky(damping * core_block + hdot(sketch.T, sketch))

    def precondition(residual):
        coeffs = factor_solve(factor, hdot(sketch.T, residual))
        result = (residual - hdot(sketch, coeffs)) / damping
        return (result, hdot(result.T, residual))

    start = lax.axis_index("samp") * rows
    solution = jnp.zeros(all_energies.shape, jnp.float32)
    update = 0.0
    residual = all_energies
    precond_res, inner_prev = precondition(residual)
    direction = precond_res
    for iteration in range(ITERS):
        rounded = lax.dynamic_slice_in_dim(direction, start, rows, 0).astype(jnp.bfloat16)
        part = jnp.einsum("rv,rc->vc", rounded, centered, preferred_element_type=jnp.float32)
        projected = reduce_all(part.astype(jnp.bfloat16), n, 2 + 2 * iteration)
        if iteration + 1 < ITERS:
            image_part = jnp.einsum("rc,vc->vr", centered, projected, preferred_element_type=jnp.float32)
            image_k = sum_and_spread(image_part, n, p, 3 + 2 * iteration)
            image_k = image_k.transpose(0, 2, 1).reshape(n * rows, count) + damping * direction
            curvature = hdot(direction.T, image_k)
        else:
            square = jnp.einsum("uc,vc->uv", projected, projected, preferred_element_type=jnp.float32)
            curvature = tiny_sum(square, p, 3 + 2 * iteration) + damping * hdot(direction.T, direction)
        alpha_k = small_solve(curvature, inner_prev)
        solution = solution + hdot(direction, alpha_k)
        update = update + hdot(alpha_k.T, projected.astype(jnp.float32))
        if iteration + 1 < ITERS:
            residual = residual - hdot(image_k, alpha_k)
            precond_res, inner_next = precondition(residual)
            beta_k = small_solve(inner_prev, inner_next)
            direction = precond_res + hdot(direction, beta_k)
            inner_prev = inner_next
    return (update.T, lax.dynamic_slice_in_dim(solution, start, rows, 0))


def solution(mesh):
    return jax.shard_map(
        body,
        mesh=mesh,
        in_specs=(P("samp", "par"), P("samp", None), P("samp", None)),
        out_specs=(P("par", None), P("samp", None)),
        check_vma=False,
    )
```

```python
import functools
import math

import jax
import jax.numpy as jnp
from jax import lax
from jax.experimental import pallas as pl
from jax.experimental.pallas import tpu as pltpu
from jax.sharding import PartitionSpec as P

ITERS = 2


damping = 0.5

MESH = pl.DeviceIdType.MESH


def factor_solve(factor, right):
    middle = lax.linalg.triangular_solve(factor, right, left_side=True, lower=True)
    return lax.linalg.triangular_solve(factor, middle, left_side=True, lower=True, transpose_a=True)


def eliminate_kernel(matrix_ref, right_ref, out_ref):
    left, right = matrix_ref[...], right_ref[...]
    row = lax.broadcasted_iota(jnp.int32, left.shape, 0)
    for i in range(left.shape[0]):
        column = left[:, i:i + 1]
        pivot = left[i:i + 1, i:i + 1]
        left_row = left[i:i + 1, :] / pivot
        right_row = right[i:i + 1, :] / pivot
        left = jnp.where(row == i, left_row, left - column * left_row)
        right = jnp.where(row == i, right_row, right - column * right_row)
    out_ref[...] = right


def small_solve(matrix, right):
    matrix = 0.5 * (matrix + matrix.T)
    return pl.pallas_call(
        eliminate_kernel, out_shape=jax.ShapeDtypeStruct(right.shape, right.dtype)
    )(matrix, right)


def hdot(left, right):
    return jnp.dot(left, right, precision=lax.Precision.HIGHEST)


def greet(peers):
    barrier = pltpu.get_barrier_semaphore()
    for peer in peers:
        pl.semaphore_signal(barrier, inc=1, device_id=peer, device_id_type=MESH)
    pl.semaphore_wait(barrier, len(peers))


def remote(src, dst, send, recv, peer):
    return pltpu.make_async_remote_copy(
        src_ref=src, dst_ref=dst, send_sem=send, recv_sem=recv, device_id=peer, device_id_type=MESH
    )


def gather_kernel(n, total_rows, scale, sums_ref, aux_ref, chosen_ref, full_ref, sketch_ref, aux_out, centered_out,
                  mean_ref, rows_out, centered_ref, land, own, full, s1, r1, s2, r2, s3, r3, s4, r4, s5, r5, s6, r6, local):
    me, col = lax.axis_index("samp"), lax.axis_index("par")
    at = [lax.rem(me + k, n) for k in range(n)]
    back = [lax.rem(me + n - k, n) for k in range(n)]
    peer = [(at[k], col) for k in range(n)]
    pair = (jnp.bitwise_xor(me, 1), col)
    width = chosen_ref.shape[1]
    half = width // 2
    part = [pl.ds(0, half), pl.ds(half, half)]
    load = pltpu.make_async_copy(full_ref, full, local.at[2])
    load.start()
    greet(peer[1:])
    scatter = [remote(sums_ref.at[at[k]], land.at[k], s1.at[k], r1.at[k], peer[k]) for k in range(1, n)]
    for copy in scatter:
        copy.start()
    sent = list(scatter)
    quad = n == 8
    beside = [jnp.bitwise_xor(me, 2), jnp.bitwise_xor(me, 4)]
    if quad:
        first = [
            remote(chosen_ref.at[:, part[d]], rows_out.at[me, :, part[d]], s4.at[d], r4.at[d], (beside[d], col))
            for d in range(2)
        ]
        for copy in first:
            copy.start()
        sent += first
    auxes = [remote(aux_ref, aux_out.at[me], s2.at[k], r2.at[k], peer[k]) for k in range(1, n)]
    mine = pltpu.make_async_copy(aux_ref, aux_out.at[me], local.at[0])
    mine.start()
    keep = pltpu.make_async_copy(chosen_ref, rows_out.at[me], local.at[1])
    keep.start()
    total = sums_ref[me]
    for k in range(1, n):
        scatter[k - 1].wait_recv()
        total = total + land[k]
    own[...] = total / total_rows
    mean_ref[me] = own[...]
    spread = [remote(own, mean_ref.at[me], s3.at[k], r3.at[k], peer[k]) for k in range(1, n)]
    for copy in spread + auxes:
        copy.start()
    sent += spread + auxes
    over = [remote(chosen_ref, rows_out.at[me], s5.at[0], r5.at[0], pair)]
    over[0].start()
    if quad:
        second = [
            remote(chosen_ref.at[:, part[1 - d]], rows_out.at[me, :, part[1 - d]], s4.at[2 + d], r4.at[2 + d],
                   (beside[d], col))
            for d in range(2)
        ]
        for copy in second:
            copy.start()
        sent += second
        for d in range(2):
            view = rows_out.at[beside[d], :, part[d]]
            remote(view, view, s4.at[d], r4.at[d], pair).wait_recv()
            step = remote(view, view, s4.at[4 + d], r4.at[4 + d], (beside[1 - d], col))
            step.start()
            sent.append(step)
    else:
        far = [remote(chosen_ref, rows_out.at[me], s4.at[k], r4.at[k], peer[k]) for k in range(2, n, 2)]
        for copy in far:
            copy.start()
        sent += far
    for k in range(1, n):
        remote(own, mean_ref.at[back[k]], s3.at[k], r3.at[k], peer[k]).wait_recv()
    load.wait()
    slab = width // n
    tile = math.gcd(slab, 1024)

    @pl.loop(0, n)
    def _(j):
        @pl.loop(0, slab // tile)
        def _(t):
            inner = pl.multiple_of(t * tile, tile)
            cols = pl.ds(pl.multiple_of(j * slab + inner, tile), tile)
            mean = mean_ref[j, :, pl.ds(inner, tile)]
            centered_ref[:, cols] = ((full[:, cols].astype(jnp.float32) - mean) * scale).astype(jnp.bfloat16)

    put = pltpu.make_async_copy(centered_ref, centered_out, local.at[2])
    put.start()
    if quad:
        for d in range(2):
            view = rows_out.at[beside[d], :, part[1 - d]]
            remote(view, view, s4.at[2 + d], r4.at[2 + d], pair).wait_recv()
            block = rows_out.at[beside[d]]
            step = remote(block, block, s5.at[1 + d], r5.at[1 + d], pair)
            step.start()
            over.append(step)
        cross = jnp.bitwise_xor(me, 6)
        for d in range(2):
            view = rows_out.at[cross, :, part[d]]
            remote(view, view, s4.at[4 + d], r4.at[4 + d], pair).wait_recv()
            step = remote(view, view, s5.at[3 + d], r5.at[3 + d], pair)
            step.start()
            over.append(step)
        block = rows_out.at[jnp.bitwise_xor(me, 1)]
        remote(block, block, s5.at[0], r5.at[0], pair).wait_recv()
        for d in range(2):
            block = rows_out.at[jnp.bitwise_xor(me, 3 + 2 * d)]
            remote(block, block, s5.at[1 + d], r5.at[1 + d], pair).wait_recv()
            view = rows_out.at[jnp.bitwise_xor(me, 7), :, part[d]]
            remote(view, view, s5.at[3 + d], r5.at[3 + d], pair).wait_recv()
    else:
        for k in range(2, n, 2):
            block = rows_out.at[back[k]]
            remote(block, block, s4.at[k], r4.at[k], pair).wait_recv()
            step = remote(block, block, s5.at[k], r5.at[k], pair)
            step.start()
            over.append(step)
        for k in range(0, n, 2):
            block = rows_out.at[lax.rem(pair[0] + n - k, n)]
            remote(block, block, s5.at[k], r5.at[k], pair).wait_recv()
    for k in range(1, n):
        remote(aux_ref, aux_out.at[back[k]], s2.at[k], r2.at[k], peer[k]).wait_recv()
    for copy in sent + over:
        copy.wait_send()
    mine.wait()
    keep.wait()
    sketch_ref[...] = jnp.zeros_like(sketch_ref)
    count = n * chosen_ref.shape[0]

    @pl.loop(0, n)
    def _(j):
        @pl.loop(0, slab // tile)
        def _(t):
            inner = pl.multiple_of(t * tile, tile)
            cols = pl.ds(pl.multiple_of(j * slab + inner, tile), tile)
            mean = mean_ref[j, :, pl.ds(inner, tile)]
            rows = rows_out[:, :, cols].astype(jnp.float32).reshape(count, tile)
            rows = ((rows - mean) * scale).astype(jnp.bfloat16)
            sketch_ref[...] += lax.dot_general(
                centered_ref[:, cols], rows, (((1,), (1,)), ((), ())), preferred_element_type=jnp.float32
            )

    put.wait()


def gather_rows(sums, aux, chosen, full, n, total_rows, scale, ident):
    dma = lambda: pltpu.SemaphoreType.DMA((n,))
    vmem = pl.BlockSpec(memory_space=pltpu.VMEM)
    slab = sums.shape[-1]
    return pl.pallas_call(
        functools.partial(gather_kernel, n, total_rows, scale),
        out_shape=(
            jax.ShapeDtypeStruct((full.shape[0], n * chosen.shape[0]), jnp.float32),
            jax.ShapeDtypeStruct((n,) + aux.shape, jnp.float32),
            jax.ShapeDtypeStruct(full.shape, full.dtype),
        ),
        in_specs=[vmem, vmem, vmem, pl.BlockSpec(memory_space=pl.ANY)],
        out_specs=(vmem, vmem, pl.BlockSpec(memory_space=pl.ANY)),
        scratch_shapes=[
            pltpu.VMEM(sums.shape, jnp.float32),
            pltpu.VMEM((n,) + chosen.shape, chosen.dtype),
            pltpu.VMEM(full.shape, full.dtype),
            pltpu.VMEM(sums.shape, jnp.float32),
            pltpu.VMEM((1, slab), jnp.float32),
            pltpu.VMEM(full.shape, full.dtype),
        ] + [dma() for _ in range(12)] + [pltpu.SemaphoreType.DMA((3,))],
        compiler_params=pltpu.CompilerParams(
            collective_id=ident, has_side_effects=True, vmem_limit_bytes=60 * 2**20
        ),
    )(sums, aux, chosen, full)


def spread_kernel(n, p, part_ref, out_ref, land, own, s1, r1, s2, r2):
    me, col = lax.axis_index("samp"), lax.axis_index("par")
    beside = [lax.rem(col + k, p) for k in range(p)]
    at = [lax.rem(me + k, n) for k in range(n)]
    back = [lax.rem(me + n - k, n) for k in range(n)]
    greet([(me, beside[k]) for k in range(1, p)] + [(at[k], col) for k in range(1, n)])
    sums = [remote(part_ref, land.at[col], s1.at[k], r1.at[k], (me, beside[k])) for k in range(1, p)]
    for copy in sums:
        copy.start()
    land[col] = part_ref[...]
    for k in range(1, p):
        there = lax.rem(col + p - k, p)
        remote(part_ref, land.at[there], s1.at[k], r1.at[k], (me, beside[k])).wait_recv()
    total = land[0]
    for j in range(1, p):
        total = total + land[j]
    own[...] = total
    out_ref[me] = total
    hops = [remote(own, out_ref.at[me], s2.at[k], r2.at[k], (at[k], col)) for k in range(1, n)]
    for copy in hops:
        copy.start()
    for k in range(1, n):
        remote(own, out_ref.at[back[k]], s2.at[k], r2.at[k], (at[k], col)).wait_recv()
    for copy in sums + hops:
        copy.wait_send()


def sum_and_spread(part, n, p, ident):
    vmem = pl.BlockSpec(memory_space=pltpu.VMEM)
    return pl.pallas_call(
        functools.partial(spread_kernel, n, p),
        out_shape=jax.ShapeDtypeStruct((n,) + part.shape, jnp.float32),
        in_specs=[vmem],
        out_specs=vmem,
        scratch_shapes=[
            pltpu.VMEM((p,) + part.shape, jnp.float32),
            pltpu.VMEM(part.shape, jnp.float32),
            pltpu.SemaphoreType.DMA((p,)),
            pltpu.SemaphoreType.DMA((p,)),
            pltpu.SemaphoreType.DMA((n,)),
            pltpu.SemaphoreType.DMA((n,)),
        ],
        compiler_params=pltpu.CompilerParams(collective_id=ident, has_side_effects=True),
    )(part)


def reduce_kernel(n, part_ref, out_ref, land, both, inbox, s0, r0, s1, r1, s2, r2, s3, r3):
    me, col = lax.axis_index("samp"), lax.axis_index("par")
    outer = n // 2
    slab = part_ref.shape[1] // n
    half = slab * outer
    i, o = lax.rem(me, 2), me // 2
    pair = (jnp.bitwise_xor(me, 1), col)
    at = [lax.rem(o + k, outer) for k in range(outer)]
    back = [lax.rem(o + outer - k, outer) for k in range(outer)]
    peer = [(at[k] * 2 + i, col) for k in range(outer)]
    cols = lambda j: pl.ds(pl.multiple_of(j * slab, slab), slab)
    halves = lambda j: pl.ds(pl.multiple_of(j * half, half), half)
    greet([pair] + peer[1:])
    swap = remote(part_ref.at[:, halves(1 - i)], land, s0.at[0], r0.at[0], pair)
    swap.start()
    swap.wait_recv()
    both[...] = (part_ref[:, halves(i)].astype(jnp.float32) + land[...].astype(jnp.float32)).astype(both.dtype)
    scatter = [remote(both.at[:, cols(at[k])], inbox.at[k], s1.at[k], r1.at[k], peer[k]) for k in range(1, outer)]
    for copy in scatter:
        copy.start()
    total = part_ref[:, cols(i * outer + o)].astype(jnp.float32) + land[:, cols(o)].astype(jnp.float32)
    for k in range(1, outer):
        scatter[k - 1].wait_recv()
        total = total + inbox[k].astype(jnp.float32)
    home = cols(i * outer + o)
    out_ref[:, home] = total.astype(out_ref.dtype)
    mine = out_ref.at[:, home]
    spread = [remote(mine, mine, s2.at[k], r2.at[k], peer[k]) for k in range(1, outer)]
    spread.append(remote(mine, mine, s3.at[0], r3.at[0], pair))
    for copy in spread:
        copy.start()
    for k in range(1, outer):
        block = out_ref.at[:, cols(i * outer + back[k])]
        remote(block, block, s2.at[k], r2.at[k], pair).wait_recv()
        step = remote(block, block, s3.at[k], r3.at[k], pair)
        step.start()
        spread.append(step)
    for k in range(outer):
        block = out_ref.at[:, cols((1 - i) * outer + back[k])]
        remote(block, block, s3.at[k], r3.at[k], pair).wait_recv()
    for copy in [swap] + scatter + spread:
        copy.wait_send()


def reduce_all(part, n, ident):
    count, width = part.shape
    outer = n // 2
    vmem = pl.BlockSpec(memory_space=pltpu.VMEM)
    return pl.pallas_call(
        functools.partial(reduce_kernel, n),
        out_shape=jax.ShapeDtypeStruct(part.shape, part.dtype),
        in_specs=[vmem],
        out_specs=vmem,
        scratch_shapes=[
            pltpu.VMEM((count, width // 2), part.dtype),
            pltpu.VMEM((count, width // 2), part.dtype),
            pltpu.VMEM((outer, count, width // n), part.dtype),
        ]
        + [pltpu.SemaphoreType.DMA((outer,)) for _ in range(8)],
        compiler_params=pltpu.CompilerParams(collective_id=ident, has_side_effects=True),
    )(part)


def tiny_kernel(p, part_ref, out_ref, land, s1, r1):
    me, col = lax.axis_index("samp"), lax.axis_index("par")
    at = [lax.rem(col + k, p) for k in range(p)]
    back = [lax.rem(col + p - k, p) for k in range(p)]
    greet([(me, at[k]) for k in range(1, p)])
    copies = [remote(part_ref, land.at[col], s1.at[k], r1.at[k], (me, at[k])) for k in range(1, p)]
    for copy in copies:
        copy.start()
    land[col] = part_ref[...]
    for k in range(1, p):
        remote(part_ref, land.at[back[k]], s1.at[k], r1.at[k], (me, at[k])).wait_recv()
    for copy in copies:
        copy.wait_send()
    total = land[0]
    for j in range(1, p):
        total = total + land[j]
    out_ref[...] = total


def tiny_sum(part, p, ident):
    vmem = pl.BlockSpec(memory_space=pltpu.VMEM)
    return pl.pallas_call(
        functools.partial(tiny_kernel, p),
        out_shape=jax.ShapeDtypeStruct(part.shape, part.dtype),
        in_specs=[vmem],
        out_specs=vmem,
        scratch_shapes=[pltpu.VMEM((p,) + part.shape, part.dtype)]
        + [pltpu.SemaphoreType.DMA((p,)) for _ in range(2)],
        compiler_params=pltpu.CompilerParams(collective_id=ident, has_side_effects=True),
    )(part)


def body(log_derivs, energies, nys_rows):
    rows, width = log_derivs.shape
    n, p = lax.axis_size("samp"), lax.axis_size("par")
    count, rank = energies.shape[1], nys_rows.shape[1]
    scale = 1.0 / math.sqrt(width * p)
    picks = (nys_rows.reshape(rank, 1) == lax.broadcasted_iota(jnp.int32, (rank, rows), 1)).astype(jnp.bfloat16)
    probe = jnp.concatenate([picks, jnp.ones((8, rows), jnp.bfloat16)], axis=0)
    taken = jnp.dot(probe, log_derivs, preferred_element_type=jnp.float32)
    chosen = taken[:rank].astype(jnp.bfloat16)
    sums = taken[rank].reshape(n, 1, width // n)
    aux = jnp.concatenate([energies, picks.astype(jnp.float32).T], axis=1)
    sketch_part, aux_all, centered = gather_rows(sums, aux, chosen, log_derivs, n, n * rows, scale, 0)
    sketch = sum_and_spread(sketch_part, n, p, 1).reshape(n * rows, n * rank)
    all_energies = aux_all[:, :, :count].reshape(n * rows, count)
    core_block = jnp.einsum(
        "grj,grk->gjk", aux_all[:, :, count:], sketch.reshape(n, rows, n * rank), precision=lax.Precision.HIGHEST
    ).reshape(n * rank, n * rank)
    factor = jnp.linalg.cholesky(damping * core_block + hdot(sketch.T, sketch))

    def precondition(residual):
        coeffs = factor_solve(factor, hdot(sketch.T, residual))
        result = (residual - hdot(sketch, coeffs)) / damping
        return (result, hdot(result.T, residual))

    start = lax.axis_index("samp") * rows
    solution = jnp.zeros(all_energies.shape, jnp.float32)
    update = 0.0
    residual = all_energies
    precond_res, inner_prev = precondition(residual)
    direction = precond_res
    for iteration in range(ITERS):
        rounded = lax.dynamic_slice_in_dim(direction, start, rows, 0).astype(jnp.bfloat16)
        part = jnp.einsum("rv,rc->vc", rounded, centered, preferred_element_type=jnp.float32)
        projected = reduce_all(part.astype(jnp.bfloat16), n, 2 + 2 * iteration)
        if iteration + 1 < ITERS:
            image_part = jnp.einsum("rc,vc->vr", centered, projected, preferred_element_type=jnp.float32)
            image_k = sum_and_spread(image_part, n, p, 3 + 2 * iteration)
            image_k = image_k.transpose(0, 2, 1).reshape(n * rows, count) + damping * direction
            curvature = hdot(direction.T, image_k)
        else:
            square = jnp.einsum("uc,vc->uv", projected, projected, preferred_element_type=jnp.float32)
            curvature = tiny_sum(square, p, 3 + 2 * iteration) + damping * hdot(direction.T, direction)
        alpha_k = small_solve(curvature, inner_prev)
        solution = solution + hdot(direction, alpha_k)
        update = update + hdot(alpha_k.T, projected.astype(jnp.float32))
        if iteration + 1 < ITERS:
            residual = residual - hdot(image_k, alpha_k)
            precond_res, inner_next = precondition(residual)
            beta_k = small_solve(inner_prev, inner_next)
            direction = precond_res + hdot(direction, beta_k)
            inner_prev = inner_next
    return (update.T, lax.dynamic_slice_in_dim(solution, start, rows, 0))


def solution(mesh):
    return jax.shard_map(
        body,
        mesh=mesh,
        in_specs=(P("samp", "par"), P("samp", None), P("samp", None)),
        out_specs=(P("par", None), P("samp", None)),
        check_vma=False,
    )
```
